32 devices in a mesh: rep: 4 (over y, x), tp: 8 (over z, core).
Axes of the slice: x: 2, y: 2, z: 4, core: 2. Of those that a mesh axis runs over, the one named last changes fastest.
Arguments:
- residual: bfloat16 [4, 1024, 4096], P('rep', 'tp'), may hold values from -6 to 6
- gate_pre: bfloat16 [4, 1024, 7168], P('rep', None, 'tp'), may hold values from -6 to 6
- up_pre: bfloat16 [4, 1024, 7168], P('rep', None, 'tp'), may hold values from -6 to 6
- down_weight: bfloat16 [7168, 4096], P('tp'), may hold values from -0.0625 to 0.0625
- d_out: bfloat16 [4, 1024, 4096], P('rep', 'tp'), may hold values from -1.5 to 1.5
- comp_index: int32 [4, 112, 2048], P('rep', 'tp'), may hold values from 0 to 4095
- comp_value: bfloat16 [4, 112, 2048], P('rep', 'tp'), may hold values from -48 to 48
Outputs:
- output: bfloat16 [4, 1024, 4096], P('rep', 'tp')
- gate_preact_gradient: bfloat16 [4, 1024, 7168], P('rep', None, 'tp')
- up_grad: bfloat16 [4, 1024, 7168], P('rep', None, 'tp')
- weight_grad: bfloat16 [4, 7168, 4096], P('rep', 'tp')
- update: bfloat16 [7168, 4096], P('tp')
- updated_down_weight: bfloat16 [7168, 4096], P('tp')
The draws below stay inside these ranges and needn't reach their ends.
Inputs may be any that keep to these rules, and one draw needn't show every extreme that they name: `comp_index`: positions of one list may repeat.
All inputs are finite; a program needn't handle non-finite values.
Results may differ from the reference program's by a relative error of at most 0.011.
Values may be sent and summed in bfloat16 or wider, within the bound.
A program may use at most 320 MiB of HBM per device.

```python
import jax
import jax.numpy as jnp
from jax import lax

D = 4096
FF = 7168
SPAN = 64
TOPK = 32
TOKENS = 1024
REPS = 4
N_REP = 4
N_TP = 8


def with_ends(drawn, key, least, largest):
    shape = drawn.shape
    spot = [jax.random.randint(jax.random.fold_in(key, axis), (), 0, shape[axis]) for axis in range(len(shape))]
    drawn = drawn.at[tuple(spot)].set(least)
    longest = shape.index(max(shape))
    spot[longest] = (spot[longest] + 1) % shape[longest]
    return drawn.at[tuple(spot)].set(largest)


def level_of(stream_key, shape, pieces, low, high):
    def one(dim, blocks):
        draws = jax.random.uniform(jax.random.fold_in(jax.random.fold_in(stream_key, 6), dim), (blocks,), jnp.float32, low / len(pieces), high / len(pieces))
        return jnp.repeat(jnp.exp(draws), shape[dim] // blocks).reshape((-1,) + (1,) * (len(shape) - dim - 1))

    level = one(*pieces[0])
    for cut in pieces[1:]:
        level = level * one(*cut)
    return level


def noise(key, extent, scale, bound, cuts=(), kind=jnp.bfloat16):
    drawn = scale * jax.random.normal(key, extent, jnp.float32)
    if cuts:
        drawn = drawn * level_of(key, extent, cuts, -0.22, 0.18)
    return jnp.clip(drawn, -bound, bound).astype(kind)


def setup_inputs(seed: int = 0) -> dict:
    keys = jax.random.split(jax.random.key(seed), 8)
    return {
        "residual": noise(keys[0], (REPS, TOKENS, D), 1.0, 6.0, ((0, 4), (1, 8))),
        "gate_pre": noise(keys[1], (REPS, TOKENS, FF), 1.0, 6.0, ((0, 4), (2, 8))),
        "up_pre": noise(keys[2], (REPS, TOKENS, FF), 1.0, 6.0, ((0, 4), (2, 8))),
        "down_weight": noise(keys[3], (FF, D), FF ** -0.5, 0.0625, ((0, 8),)),
        "d_out": noise(keys[4], (REPS, TOKENS, D), 0.25, 1.5, ((0, 4), (1, 8))),
        "comp_index": with_ends(jax.random.randint(keys[5], (REPS, FF // SPAN, (D // SPAN) * TOPK), 0, SPAN * SPAN), jax.random.fold_in(keys[5], 1), 0, (SPAN * SPAN) - 1).astype(jnp.int32),
        "comp_value": noise(keys[6], (REPS, FF // SPAN, (D // SPAN) * TOPK), 8.0, 48.0, ((0, 4), (1, 8))),
    }


def cosine_table(length):
    freq = jnp.arange(length, dtype=jnp.float32)[:, None]
    place = jnp.arange(length, dtype=jnp.float32)[None, :]
    scales = jnp.where(freq == 0, jnp.sqrt(1.0 / length), jnp.sqrt(2.0 / length))
    return scales * jnp.cos(jnp.pi * (2.0 * place + 1.0) * freq / (2.0 * length))

def reference(residual, gate_pre, up_pre, down_weight, d_out, comp_index, comp_value):
    units = FF // N_TP

    def per_replica(operands):
        residual_r, gate_r, up_r, grads_r = operands
        gate_f = gate_r.astype(jnp.float32)
        up_f = up_r.astype(jnp.float32)
        sigmoid_g = jax.nn.sigmoid(gate_f)
        activated = gate_f * sigmoid_g
        hidden = (activated * up_f).astype(jnp.bfloat16)
        summed = jnp.zeros((TOKENS, D), jnp.float32)
        for shard in range(N_TP):
            partial_out = jnp.dot(hidden[:, shard * units:(shard + 1) * units], down_weight[shard * units:(shard + 1) * units], preferred_element_type=jnp.float32)
            summed = summed + lax.optimization_barrier(partial_out.astype(jnp.bfloat16)).astype(jnp.float32)
        output = (residual_r.astype(jnp.float32) + summed).astype(jnp.bfloat16)
        hidden_grad = jnp.dot(grads_r, down_weight.T, preferred_element_type=jnp.float32)
        gate_preact_gradient = (hidden_grad * up_f * sigmoid_g * (1.0 + gate_f * (1.0 - sigmoid_g))).astype(jnp.bfloat16)
        up_grad = (hidden_grad * activated).astype(jnp.bfloat16)
        weight_grad = jnp.dot(hidden.T, grads_r, preferred_element_type=jnp.float32).astype(jnp.bfloat16)
        return (output, gate_preact_gradient, up_grad, weight_grad)
    output, gate_preact_gradient, up_grad, weight_grad = lax.map(per_replica, (residual, gate_pre, up_pre, d_out))
    cosine_basis = cosine_table(SPAN)
    columns = D // SPAN
    owners = jnp.broadcast_to((jnp.arange(columns * TOPK) // TOPK).astype(jnp.int32)[None, :], (N_REP, columns * TOPK))

    def span_row(operands):
        indices, amounts = operands
        flat = jnp.zeros((columns, SPAN * SPAN), jnp.float32).at[owners, indices.astype(jnp.int32)].add(amounts.astype(jnp.float32))
        spectral_coefficients = flat.reshape(columns, SPAN, SPAN)
        halfway_finished = jnp.einsum('kxt,ta->kxa', spectral_coefficients, cosine_basis, precision=lax.Precision.HIGHEST)
        output_block_list = jnp.einsum('nk,hnm->khm', cosine_basis, halfway_finished, precision=lax.Precision.HIGHEST)
        return output_block_list.reshape(SPAN, D)
    decoded = lax.map(span_row, (jnp.transpose(comp_index, (1, 0, 2)), jnp.transpose(comp_value, (1, 0, 2))))
    update = (decoded.reshape(FF, D) / N_REP).astype(jnp.bfloat16)
    updated_down_weight = (down_weight.astype(jnp.float32) - 0.02 * update.astype(jnp.float32)).astype(jnp.bfloat16)
    return (output, gate_preact_gradient, up_grad, weight_grad, update, updated_down_weight)
```

```python
import functools

import jax
import jax.numpy as jnp
import numpy as np
from jax import lax
from jax.experimental import pallas as pl
from jax.experimental.pallas import tpu as pltpu
from jax.sharding import PartitionSpec as P

SPAN = 64
TOPK = 32


learn_rate = 0.02


LANES = 128


def cosine_table(length):
    freq = np.arange(length, dtype=np.float64)[:, None]
    place = np.arange(length, dtype=np.float64)[None, :]
    scales = np.where(freq == 0, np.sqrt(1.0 / length), np.sqrt(2.0 / length))
    return scales * np.cos(np.pi * (2.0 * place + 1.0) * freq / (2.0 * length))


def decode_kernel(count, *refs):
    index_refs, value_refs = refs[:count], refs[count:2 * count]
    weight_ref, right_ref, left_ref, update_ref, weight_out_ref, mixed_ref = refs[2 * count:]
    groups = index_refs[0].shape[1] // LANES
    per_group = LANES // TOPK
    width = per_group * SPAN
    depth = count * LANES
    lane = lax.broadcasted_iota(jnp.int32, (1, depth), 1)
    shift = ((lane // TOPK) % per_group) * SPAN
    row_place = lax.broadcasted_iota(jnp.int32, (SPAN, depth), 0).astype(jnp.float32).astype(jnp.bfloat16)
    col_place = lax.broadcasted_iota(jnp.int32, (width, depth), 0).astype(jnp.float32).astype(jnp.bfloat16)

    def gather(group, carry):
        at = pl.ds(pl.multiple_of(group * LANES, LANES), LANES)
        words = jnp.concatenate([ref[:, at] for ref in index_refs], axis=1)
        values = jnp.concatenate([ref[:, at] for ref in value_refs], axis=1).astype(jnp.bfloat16)
        rows = (words >> (SPAN.bit_length() - 1)).astype(jnp.float32).astype(jnp.bfloat16)
        cols = ((words & (SPAN - 1)) + shift).astype(jnp.float32).astype(jnp.bfloat16)
        row_hot = jnp.where(rows == row_place, values, jnp.bfloat16(0))
        col_hot = jnp.where(cols == col_place, jnp.bfloat16(1), jnp.bfloat16(0))
        spectral = lax.dot_general(
            row_hot, col_hot, (((1,), (1,)), ((), ())), preferred_element_type=jnp.float32
        )
        mixed_ref[pl.ds(pl.multiple_of(group * SPAN, SPAN), SPAN), :] = spectral.astype(jnp.bfloat16)
        return carry

    lax.fori_loop(0, groups, gather, 0, unroll=UNROLL)
    halfway = jnp.dot(
        mixed_ref[...], right_ref[...], preferred_element_type=jnp.float32
    ).astype(jnp.bfloat16)
    for group in range(groups):
        block = jnp.dot(
            left_ref[...], halfway[group * SPAN:(group + 1) * SPAN], preferred_element_type=jnp.float32
        )
        change = (block * (1.0 / count)).astype(jnp.bfloat16)
        at = slice(group * width, (group + 1) * width)
        update_ref[:, at] = change
        weight_out_ref[:, at] = (
            weight_ref[:, at].astype(jnp.float32) - learn_rate * change.astype(jnp.float32)
        ).astype(jnp.bfloat16)


UNROLL = 4


def decode(indices, values, down_weight):
    count = len(indices)
    span_rows, _, listed = indices[0].shape
    units, model = down_weight.shape
    basis = cosine_table(SPAN)
    per_group = LANES // TOPK
    width = per_group * SPAN
    right = jnp.asarray(np.kron(np.eye(per_group), basis), jnp.bfloat16)
    left = jnp.asarray(basis.T, jnp.bfloat16)
    strip = pl.BlockSpec((SPAN, model), lambda a: (a, 0))
    whole = lambda shape: pl.BlockSpec(shape, lambda a: (0, 0))
    return pl.pallas_call(
        functools.partial(decode_kernel, count),
        grid=(span_rows,),
        out_shape=[jax.ShapeDtypeStruct((units, model), jnp.bfloat16)] * 2,
        in_specs=[pl.BlockSpec((None, 1, listed), lambda a: (a, 0, 0))] * (2 * count)
        + [strip, whole((width, width)), whole((SPAN, SPAN))],
        out_specs=[strip, strip],
        scratch_shapes=[pltpu.VMEM((listed // LANES * SPAN, width), jnp.bfloat16)],
        compiler_params=pltpu.CompilerParams(
            dimension_semantics=("arbitrary",), vmem_limit_bytes=24 * 2**20
        ),
        cost_estimate=pl.CostEstimate(
            flops=20 * 10**9, bytes_accessed=units * model * 6, transcendentals=0
        ),
        name="decode",
    )(*indices, *values, down_weight, right, left)


def shards(residual, gate_pre, up_pre, down_weight, d_out, comp_index, comp_value):
    residual_r = residual[0]
    gate_r = gate_pre[0]
    up_r = up_pre[0]
    grads_r = d_out[0]
    replicas = lax.axis_size("rep")

    def from_replicas(mine):
        return [mine] + [
            lax.ppermute(mine, "rep", [(i, (i + step) % replicas) for i in range(replicas)])
            for step in range(1, replicas)
        ]

    indices = from_replicas(comp_index[0][:, None])
    values = from_replicas(comp_value[0].astype(jnp.float32)[:, None])
    gate_f = gate_r.astype(jnp.float32)
    up_f = up_r.astype(jnp.float32)
    sigmoid_g = jax.nn.sigmoid(gate_f)
    activated = gate_f * sigmoid_g
    hidden = (activated * up_f).astype(jnp.bfloat16)
    summed = lax.psum_scatter(
        jnp.dot(hidden, down_weight, preferred_element_type=jnp.float32).astype(jnp.bfloat16),
        "tp",
        scatter_dimension=0,
        tiled=True,
    ).astype(jnp.float32)
    incoming = lax.all_gather(grads_r, "tp", axis=0, tiled=True)
    from_out = lax.dot_general(
        incoming, down_weight, (((1,), (1,)), ((), ())), preferred_element_type=jnp.float32
    )
    hidden_grad = from_out
    weight_sum = lax.dot_general(
        hidden, incoming, (((0,), (0,)), ((), ())), preferred_element_type=jnp.float32
    )
    weight_sum, hidden_grad = (weight_sum, hidden_grad)
    output = (residual_r.astype(jnp.float32) + summed).astype(jnp.bfloat16)
    gate_preact_gradient = (
        hidden_grad * up_f * sigmoid_g * (1.0 + gate_f * (1.0 - sigmoid_g))
    ).astype(jnp.bfloat16)
    up_grad = (hidden_grad * activated).astype(jnp.bfloat16)
    update, updated_down_weight = decode(indices, values, down_weight)
    return (
        output[None],
        gate_preact_gradient[None],
        up_grad[None],
        weight_sum.astype(jnp.bfloat16)[None],
        update,
        updated_down_weight,
    )


def solution(mesh):
    return jax.shard_map(
        shards,
        mesh=mesh,
        in_specs=(
            P("rep", "tp", None),
            P("rep", None, "tp"),
            P("rep", None, "tp"),
            P("tp", None),
            P("rep", "tp", None),
            P("rep", "tp", None),
            P("rep", "tp", None),
        ),
        out_specs=(
            P("rep", "tp", None),
            P("rep", None, "tp"),
            P("rep", None, "tp"),
            P("rep", "tp", None),
            P("tp", None),
            P("tp", None),
        ),
        check_vma=False,
    )
```

```python
import functools

import jax
import jax.numpy as jnp
import numpy as np
from jax import lax
from jax.experimental import pallas as pl
from jax.experimental.pallas import tpu as pltpu
from jax.sharding import PartitionSpec as P

SPAN = 64
TOPK = 32


learn_rate = 0.02


LANES = 128


def cosine_table(length):
    freq = np.arange(length, dtype=np.float64)[:, None]
    place = np.arange(length, dtype=np.float64)[None, :]
    scales = np.where(freq == 0, np.sqrt(1.0 / length), np.sqrt(2.0 / length))
    return scales * np.cos(np.pi * (2.0 * place + 1.0) * freq / (2.0 * length))


def decode_kernel(count, *refs):
    index_refs, value_refs = refs[:count], refs[count:2 * count]
    weight_ref, right_ref, left_ref = refs[2 * count:2 * count + 3]
    update_ref, weight_out_ref, mixed_ref = refs[-3:]
    groups = index_refs[0].shape[1] // LANES
    per_group = LANES // TOPK
    width = per_group * SPAN
    depth = count * LANES
    lane = lax.broadcasted_iota(jnp.int32, (1, depth), 1)
    shift = ((lane // TOPK) % per_group) * SPAN
    row_place = lax.broadcasted_iota(jnp.int32, (SPAN, depth), 0).astype(jnp.float32).astype(jnp.bfloat16)
    col_place = lax.broadcasted_iota(jnp.int32, (width, depth), 0).astype(jnp.float32).astype(jnp.bfloat16)

    def gather(group, carry):
        at = pl.ds(pl.multiple_of(group * LANES, LANES), LANES)
        words = jnp.concatenate([ref[:, at] for ref in index_refs], axis=1)
        values = jnp.concatenate([ref[:, at] for ref in value_refs], axis=1).astype(jnp.bfloat16)
        rows = (words >> (SPAN.bit_length() - 1)).astype(jnp.float32).astype(jnp.bfloat16)
        cols = ((words & (SPAN - 1)) + shift).astype(jnp.float32).astype(jnp.bfloat16)
        row_hot = jnp.where(rows == row_place, values, jnp.bfloat16(0))
        col_hot = jnp.where(cols == col_place, jnp.bfloat16(1), jnp.bfloat16(0))
        spectral = lax.dot_general(
            row_hot, col_hot, (((1,), (1,)), ((), ())), preferred_element_type=jnp.float32
        )
        mixed_ref[pl.ds(pl.multiple_of(group * SPAN, SPAN), SPAN), :] = spectral.astype(jnp.bfloat16)
        return carry

    lax.fori_loop(0, groups, gather, 0, unroll=UNROLL)
    halfway = jnp.dot(
        mixed_ref[...], right_ref[...], preferred_element_type=jnp.float32
    ).astype(jnp.bfloat16)
    for group in range(groups):
        block = jnp.dot(
            left_ref[...], halfway[group * SPAN:(group + 1) * SPAN], preferred_element_type=jnp.float32
        )
        change = (block * (1.0 / count)).astype(jnp.bfloat16)
        at = slice(group * width, (group + 1) * width)
        update_ref[:, at] = change
        weight_out_ref[:, at] = (
            weight_ref[:, at].astype(jnp.float32) - learn_rate * change.astype(jnp.float32)
        ).astype(jnp.bfloat16)


UNROLL = 4


def decode(indices, values, down_weight):
    span_rows = indices[0].shape[0]
    first = span_rows // 2
    done = decode_rows(indices, values, down_weight, 0, first, ())
    return decode_rows(indices, values, down_weight, first, span_rows - first, done)


def decode_rows(indices, values, down_weight, first, held, done):
    count = len(indices)
    listed = indices[0].shape[2]
    units, model = down_weight.shape
    basis = cosine_table(SPAN)
    per_group = LANES // TOPK
    width = per_group * SPAN
    right = jnp.asarray(np.kron(np.eye(per_group), basis), jnp.bfloat16)
    left = jnp.asarray(basis.T, jnp.bfloat16)
    strip = pl.BlockSpec((SPAN, model), lambda a: (a + first, 0))
    whole = lambda shape: pl.BlockSpec(shape, lambda a: (0, 0))
    return pl.pallas_call(
        functools.partial(decode_kernel, count),
        grid=(held,),
        out_shape=[jax.ShapeDtypeStruct((units, model), jnp.bfloat16)] * 2,
        in_specs=[pl.BlockSpec((None, 1, listed), lambda a: (a + first, 0, 0))] * (2 * count)
        + [strip, whole((width, width)), whole((SPAN, SPAN))]
        + [pl.BlockSpec(memory_space=pl.ANY)] * len(done),
        out_specs=[strip, strip],
        scratch_shapes=[pltpu.VMEM((listed // LANES * SPAN, width), jnp.bfloat16)],
        compiler_params=pltpu.CompilerParams(
            dimension_semantics=("arbitrary",), vmem_limit_bytes=24 * 2**20
        ),
        cost_estimate=pl.CostEstimate(
            flops=14 * 10**8 * held, bytes_accessed=held * SPAN * model * 6, transcendentals=0
        ),
        input_output_aliases={2 * count + 3 + i: i for i in range(len(done))},
        name="decode",
    )(*indices, *values, down_weight, right, left, *done)


def shifted(block, stride):
    size = lax.axis_size("tp")
    return lax.ppermute(block, "tp", [(i, (i + stride) % size) for i in range(size)])


def swapped(block):
    return lax.ppermute(block, "tp", [(i, i ^ 1) for i in range(lax.axis_size("tp"))])


def ring_pieces(block):
    chips = lax.axis_size("tp") // 2
    half = block.shape[0] // 2
    upward = downward = block
    pieces = [(0, 0, block)]
    for step in range(1, (chips - 1) // 2 + 1):
        upward, downward = shifted(upward, 2), shifted(downward, -2)
        pieces += [(-step, 0, upward), (step, 0, downward)]
    if chips % 2 == 0:
        pieces += [
            (chips // 2, 0, shifted(upward[:half], 2)),
            (chips // 2, half, shifted(downward[half:], -2)),
        ]
    return pieces


def pair_gather(pieces):
    size = lax.axis_size("tp")
    me = lax.axis_index("tp")
    rows, columns = pieces[0][2].shape
    whole = jnp.zeros((size * rows, columns), pieces[0][2].dtype)
    for offset, start, piece in pieces:
        owner = (me + 2 * offset) % size
        for held, home in ((piece, owner), (swapped(piece), owner ^ 1)):
            whole = lax.dynamic_update_slice(whole, held, (home * rows + start, 0))
    return whole


def pair_ring_scatter(partial):
    size = lax.axis_size("tp")
    me = lax.axis_index("tp")
    chips = size // 2
    blocks = partial.reshape(chips, 2, partial.shape[0] // size, partial.shape[1])
    half = blocks.shape[2] // 2
    core = me % 2
    given = swapped(lax.dynamic_index_in_dim(blocks, 1 - core, 1, keepdims=False))
    kept = lax.dynamic_index_in_dim(blocks, core, 1, keepdims=False)

    def pair(offset):
        chip = (me // 2 + offset) % chips
        return sum(
            lax.dynamic_index_in_dim(part, chip, 0, keepdims=False).astype(jnp.float32)
            for part in (kept, given)
        )

    total = pair(0)
    for sign in (1, -1):
        arrived = None
        for distance in range(chips // 2, 0, -1):
            outgoing = pair(sign * distance)
            if chips % 2 == 0 and distance == chips // 2:
                outgoing = outgoing[:half] if sign > 0 else outgoing[half:]
            elif arrived is not None:
                outgoing = outgoing + spread(arrived, sign, outgoing.shape[0])
            arrived = shifted(outgoing.astype(jnp.bfloat16), 2 * sign)
        if arrived is not None:
            total = total + spread(arrived, sign, total.shape[0])
    return total


def spread(block, sign, rows):
    block = block.astype(jnp.float32)
    missing = rows - block.shape[0]
    return jnp.pad(block, ((0, missing), (0, 0)) if sign > 0 else ((missing, 0), (0, 0)))


def shards(residual, gate_pre, up_pre, down_weight, d_out, comp_index, comp_value):
    residual_r = residual[0]
    gate_r = gate_pre[0]
    up_r = up_pre[0]
    grads_r = d_out[0]
    replicas = lax.axis_size("rep")

    def from_replicas(mine):
        return [mine] + [
            lax.ppermute(mine, "rep", [(i, (i + step) % replicas) for i in range(replicas)])
            for step in range(1, replicas)
        ]

    indices = from_replicas(comp_index[0][:, None])
    values = from_replicas(comp_value[0].astype(jnp.float32)[:, None])
    pieces = ring_pieces(grads_r)
    gate_f = gate_r.astype(jnp.float32)
    up_f = up_r.astype(jnp.float32)
    sigmoid_g = jax.nn.sigmoid(gate_f)
    activated = gate_f * sigmoid_g
    hidden = (activated * up_f).astype(jnp.bfloat16)
    summed = pair_ring_scatter(
        jnp.dot(hidden, down_weight, preferred_element_type=jnp.float32).astype(jnp.bfloat16)
    )
    incoming = pair_gather(pieces)
    from_out = lax.dot_general(
        incoming, down_weight, (((1,), (1,)), ((), ())), preferred_element_type=jnp.float32
    )
    hidden_grad = from_out
    weight_sum = lax.dot_general(
        hidden, incoming, (((0,), (0,)), ((), ())), preferred_element_type=jnp.float32
    )
    weight_sum, hidden_grad = (weight_sum, hidden_grad)
    output = (residual_r.astype(jnp.float32) + summed).astype(jnp.bfloat16)
    gate_preact_gradient = (
        hidden_grad * up_f * sigmoid_g * (1.0 + gate_f * (1.0 - sigmoid_g))
    ).astype(jnp.bfloat16)
    up_grad = (hidden_grad * activated).astype(jnp.bfloat16)
    update, updated_down_weight = decode(indices, values, down_weight)
    return (
        output[None],
        gate_preact_gradient[None],
        up_grad[None],
        weight_sum.astype(jnp.bfloat16)[None],
        update,
        updated_down_weight,
    )


def solution(mesh):
    return jax.shard_map(
        shards,
        mesh=mesh,
        in_specs=(
            P("rep", "tp", None),
            P("rep", None, "tp"),
            P("rep", None, "tp"),
            P("tp", None),
            P("rep", "tp", None),
            P("rep", "tp", None),
            P("rep", "tp", None),
        ),
        out_specs=(
            P("rep", "tp", None),
            P("rep", None, "tp"),
            P("rep", None, "tp"),
            P("rep", "tp", None),
            P("tp", None),
            P("tp", None),
        ),
        check_vma=False,
    )
```

```python
import functools

import jax
import jax.numpy as jnp
import numpy as np
from jax import lax
from jax.experimental import pallas as pl
from jax.experimental.pallas import tpu as pltpu
from jax.sharding import PartitionSpec as P

SPAN = 64
TOPK = 32


learn_rate = 0.02


LANES = 128


def cosine_table(length):
    freq = np.arange(length, dtype=np.float64)[:, None]
    place = np.arange(length, dtype=np.float64)[None, :]
    scales = np.where(freq == 0, np.sqrt(1.0 / length), np.sqrt(2.0 / length))
    return scales * np.cos(np.pi * (2.0 * place + 1.0) * freq / (2.0 * length))


def decode_kernel(count, *refs):
    index_refs, value_refs = refs[:count], refs[count:2 * count]
    weight_ref, right_ref, left_ref = refs[2 * count:2 * count + 3]
    update_ref, weight_out_ref, mixed_ref = refs[-3:]
    groups = index_refs[0].shape[1] // LANES
    per_group = LANES // TOPK
    width = per_group * SPAN
    depth = count * LANES
    lane = lax.broadcasted_iota(jnp.int32, (1, depth), 1)
    shift = ((lane // TOPK) % per_group) * SPAN
    row_place = lax.broadcasted_iota(jnp.int32, (SPAN, depth), 0).astype(jnp.float32).astype(jnp.bfloat16)
    col_place = lax.broadcasted_iota(jnp.int32, (width, depth), 0).astype(jnp.float32).astype(jnp.bfloat16)

    def gather(group, carry):
        at = pl.ds(pl.multiple_of(group * LANES, LANES), LANES)
        words = jnp.concatenate([ref[:, at] for ref in index_refs], axis=1)
        values = jnp.concatenate([ref[:, at] for ref in value_refs], axis=1).astype(jnp.bfloat16)
        rows = (words >> (SPAN.bit_length() - 1)).astype(jnp.float32).astype(jnp.bfloat16)
        cols = ((words & (SPAN - 1)) + shift).astype(jnp.float32).astype(jnp.bfloat16)
        row_hot = jnp.where(rows == row_place, values, jnp.bfloat16(0))
        col_hot = jnp.where(cols == col_place, jnp.bfloat16(1), jnp.bfloat16(0))
        spectral = lax.dot_general(
            row_hot, col_hot, (((1,), (1,)), ((), ())), preferred_element_type=jnp.float32
        )
        mixed_ref[pl.ds(pl.multiple_of(group * SPAN, SPAN), SPAN), :] = spectral.astype(jnp.bfloat16)
        return carry

    lax.fori_loop(0, groups, gather, 0, unroll=UNROLL)
    halfway = jnp.dot(
        mixed_ref[...], right_ref[...], preferred_element_type=jnp.float32
    ).astype(jnp.bfloat16)
    for group in range(groups):
        block = jnp.dot(
            left_ref[...], halfway[group * SPAN:(group + 1) * SPAN], preferred_element_type=jnp.float32
        )
        change = (block * (1.0 / count)).astype(jnp.bfloat16)
        at = slice(group * width, (group + 1) * width)
        update_ref[:, at] = change
        weight_out_ref[:, at] = (
            weight_ref[:, at].astype(jnp.float32) - learn_rate * change.astype(jnp.float32)
        ).astype(jnp.bfloat16)


UNROLL = 4


def decode(indices, values, down_weight, step, parts, done):
    span_rows = indices[0].shape[0]
    first, end = span_rows * step // parts, span_rows * (step + 1) // parts
    return decode_rows(indices, values, down_weight, first, end - first, done)


def decode_rows(indices, values, down_weight, first, held, done):
    count = len(indices)
    listed = indices[0].shape[2]
    units, model = down_weight.shape
    basis = cosine_table(SPAN)
    per_group = LANES // TOPK
    width = per_group * SPAN
    right = jnp.asarray(np.kron(np.eye(per_group), basis), jnp.bfloat16)
    left = jnp.asarray(basis.T, jnp.bfloat16)
    strip = pl.BlockSpec((SPAN, model), lambda a: (a + first, 0))
    whole = lambda shape: pl.BlockSpec(shape, lambda a: (0, 0))
    return pl.pallas_call(
        functools.partial(decode_kernel, count),
        grid=(held,),
        out_shape=[jax.ShapeDtypeStruct((units, model), jnp.bfloat16)] * 2,
        in_specs=[pl.BlockSpec((None, 1, listed), lambda a: (a + first, 0, 0))] * (2 * count)
        + [strip, whole((width, width)), whole((SPAN, SPAN))]
        + [pl.BlockSpec(memory_space=pl.ANY)] * len(done),
        out_specs=[strip, strip],
        scratch_shapes=[pltpu.VMEM((listed // LANES * SPAN, width), jnp.bfloat16)],
        compiler_params=pltpu.CompilerParams(
            dimension_semantics=("arbitrary",), vmem_limit_bytes=24 * 2**20
        ),
        cost_estimate=pl.CostEstimate(
            flops=14 * 10**8 * held, bytes_accessed=held * SPAN * model * 6, transcendentals=0
        ),
        input_output_aliases={2 * count + 3 + i: i for i in range(len(done))},
        name="decode",
    )(*indices, *values, down_weight, right, left, *done)


def shifted(block, stride):
    size = lax.axis_size("tp")
    return lax.ppermute(block, "tp", [(i, (i + stride) % size) for i in range(size)])


def swapped(block):
    return lax.ppermute(block, "tp", [(i, i ^ 1) for i in range(lax.axis_size("tp"))])


def ring_pieces(block):
    chips = lax.axis_size("tp") // 2
    half = block.shape[0] // 2
    upward = downward = block
    pieces = [(0, 0, block)]
    for step in range(1, (chips - 1) // 2 + 1):
        upward, downward = shifted(upward, 2), shifted(downward, -2)
        pieces += [(-step, 0, upward), (step, 0, downward)]
    return pieces, (upward[:half], downward[half:])


def ring_finish(pieces, last):
    chips = lax.axis_size("tp") // 2
    if chips % 2 == 0:
        pieces = pieces + [
            (chips // 2, 0, shifted(last[0], 2)),
            (chips // 2, last[0].shape[0], shifted(last[1], -2)),
        ]
    return pieces


def pair_gather(pieces):
    size = lax.axis_size("tp")
    me = lax.axis_index("tp")
    rows, columns = pieces[0][2].shape
    whole = jnp.zeros((size * rows, columns), pieces[0][2].dtype)
    for offset, start, piece in pieces:
        owner = (me + 2 * offset) % size
        for held, home in ((piece, owner), (swapped(piece), owner ^ 1)):
            whole = lax.dynamic_update_slice(whole, held, (home * rows + start, 0))
    return whole


def pair_ring_scatter(partial, indices, values, down_weight, last):
    size = lax.axis_size("tp")
    me = lax.axis_index("tp")
    chips = size // 2
    blocks = partial.reshape(chips, 2, partial.shape[0] // size, partial.shape[1])
    half = blocks.shape[2] // 2
    core = me % 2
    given = swapped(lax.dynamic_index_in_dim(blocks, 1 - core, 1, keepdims=False))
    kept = lax.dynamic_index_in_dim(blocks, core, 1, keepdims=False)

    def pair(offset):
        chip = (me // 2 + offset) % chips
        return sum(
            lax.dynamic_index_in_dim(part, chip, 0, keepdims=False).astype(jnp.float32)
            for part in (kept, given)
        )

    done = ()
    arrived = {}
    parts = 2
    for step, distance in enumerate(range(chips // 2, 0, -1)):
        outgoing = []
        for sign in (1, -1):
            block = pair(sign * distance)
            if step == 0 and chips % 2 == 0:
                block = block[:half] if sign > 0 else block[half:]
            elif step > 0:
                block = block + spread(arrived[sign], sign, block.shape[0])
            outgoing.append(block.astype(jnp.bfloat16))
        if step == 0:
            outgoing, indices = lax.optimization_barrier((outgoing, indices))
        elif step == 1:
            outgoing, done, last = lax.optimization_barrier((outgoing, done, last))
        arrived = {sign: shifted(block, 2 * sign) for sign, block in zip((1, -1), outgoing)}
        if step < parts:
            done = decode(indices, values, down_weight, step, parts, done)
    for step in range(min(parts, chips // 2), parts):
        done = decode(indices, values, down_weight, step, parts, done)
    total = pair(0)
    for sign, block in arrived.items():
        total = total + spread(block, sign, total.shape[0])
    return total, last, done


def spread(block, sign, rows):
    block = block.astype(jnp.float32)
    missing = rows - block.shape[0]
    return jnp.pad(block, ((0, missing), (0, 0)) if sign > 0 else ((missing, 0), (0, 0)))


def shards(residual, gate_pre, up_pre, down_weight, d_out, comp_index, comp_value):
    residual_r = residual[0]
    gate_r = gate_pre[0]
    up_r = up_pre[0]
    grads_r = d_out[0]
    replicas = lax.axis_size("rep")

    def from_replicas(mine):
        return [mine] + [
            lax.ppermute(mine, "rep", [(i, (i + step) % replicas) for i in range(replicas)])
            for step in range(1, replicas)
        ]

    indices = from_replicas(comp_index[0][:, None])
    values = from_replicas(comp_value[0].astype(jnp.float32)[:, None])
    pieces, last = ring_pieces(grads_r)
    gate_f = gate_r.astype(jnp.float32)
    up_f = up_r.astype(jnp.float32)
    sigmoid_g = jax.nn.sigmoid(gate_f)
    activated = gate_f * sigmoid_g
    hidden = (activated * up_f).astype(jnp.bfloat16)
    summed, last, (update, updated_down_weight) = pair_ring_scatter(
        jnp.dot(hidden, down_weight, preferred_element_type=jnp.float32).astype(jnp.bfloat16),
        indices,
        values,
        down_weight,
        last,
    )
    incoming = pair_gather(ring_finish(pieces, last))
    from_out = lax.dot_general(
        incoming, down_weight, (((1,), (1,)), ((), ())), preferred_element_type=jnp.float32
    )
    hidden_grad = from_out
    weight_sum = lax.dot_general(
        hidden, incoming, (((0,), (0,)), ((), ())), preferred_element_type=jnp.float32
    )
    weight_sum, hidden_grad = (weight_sum, hidden_grad)
    output = (residual_r.astype(jnp.float32) + summed).astype(jnp.bfloat16)
    gate_preact_gradient = (
        hidden_grad * up_f * sigmoid_g * (1.0 + gate_f * (1.0 - sigmoid_g))
    ).astype(jnp.bfloat16)
    up_grad = (hidden_grad * activated).astype(jnp.bfloat16)
    return (
        output[None],
        gate_preact_gradient[None],
        up_grad[None],
        weight_sum.astype(jnp.bfloat16)[None],
        update,
        updated_down_weight,
    )


def solution(mesh):
    return jax.shard_map(
        shards,
        mesh=mesh,
        in_specs=(
            P("rep", "tp", None),
            P("rep", None, "tp"),
            P("rep", None, "tp"),
            P("tp", None),
            P("rep", "tp", None),
            P("rep", "tp", None),
            P("rep", "tp", None),
        ),
        out_specs=(
            P("rep", "tp", None),
            P("rep", None, "tp"),
            P("rep", None, "tp"),
            P("rep", "tp", None),
            P("tp", None),
            P("tp", None),
        ),
        check_vma=False,
    )
```
